32 devices in a mesh: grp: 2 (over y), lon: 4 (over x, core), lat: 4 (over z).
Axes of the slice: x: 2, y: 2, z: 4, core: 2. Of those that a mesh axis runs over, the one named last changes fastest.
Arguments:
- tracers: float32 [4, 64, 128, 128], P('grp', 'lat', 'lon'), parts along dimension 0, may hold values from -6 to 6
- adjoint_in: float32 [4, 64, 128, 128], P('grp', 'lat', 'lon'), parts along dimension 0, may hold values from -6 to 6
- shifts: int32 [2, 64], replicated, may hold values from 0 to 127, as said below
- fractions: float32 [2, 64], replicated, may hold values from 0.05 to 0.95
- meridional: float32 [2, 64, 128], P(None, None, 'lon'), may hold values from -0.9 to 0.9
Outputs:
- advected: float32 [4, 64, 128, 128], P('grp', 'lat', 'lon'), parts along dimension 0
- adjoint_out: float32 [4, 64, 128, 128], P('grp', 'lat', 'lon'), parts along dimension 0
The draws below stay inside these ranges and needn't reach their ends.
There are 2 independent parts, one for each index of `grp`. The reference program is written for one: setup_inputs(seed, part) draws one part's arguments, and reference() takes and returns one part's arrays. A program takes and returns all parts, laid end to end along the dimension named above; an argument that names none is the same for every part. Nothing has to cross between parts.
Inputs may be any that keep to these rules, and one draw needn't show every extreme that they name: At row j, shifts lie below 1 + (127) d^2 / 63^2 with d = |2j - 63|.
All inputs are finite; a program needn't handle non-finite values.
Results may differ from the reference program's by a relative error of at most 0.0003.
Values sent between devices are 32-bit elements; how exact they have to be, the bound alone decides.
A program may use at most 128 MiB of HBM per device.

```python
import jax
import jax.numpy as jnp
from jax import lax

C = 128
LEV = 2
NX = 128
NY = 64


def draw_shifts(key, part):
    row_ids = jnp.arange(NY, dtype=jnp.int32)
    distance = jnp.abs(2 * row_ids + 1 - NY)
    ceiling = 1 + (NX - 1) * distance * distance // ((NY - 1) * (NY - 1))
    drawn = jax.random.randint(key, (LEV, NY), 0, ceiling[None, :], dtype=jnp.int32)
    drawn = drawn.at[0, 0].set(NX - 1)
    drawn = drawn.at[0, NY // 2].set(0)
    return drawn


def steps_of(own_key, extent, shards, least, largest):
    level = 1.0
    for axis_at, shards_of in shards:
        draws = jax.random.uniform(jax.random.fold_in(jax.random.fold_in(own_key, 6), axis_at), (shards_of,), jnp.float32, least / len(shards), largest / len(shards))
        level = level * jnp.repeat(jnp.exp(draws), extent[axis_at] // shards_of).reshape((-1,) + (1,) * (len(extent) - 1 - axis_at))
    return level


def noise(stream_key, dims, scale, reach, pieces=(), kind=jnp.bfloat16):
    values = scale * jax.random.normal(stream_key, dims, jnp.float32)
    if pieces:
        values = values * steps_of(stream_key, dims, pieces, -0.22, 0.18)
    return jnp.clip(values, -reach, reach).astype(kind)


def setup_inputs(seed: int = 0, part: int = 0) -> dict:
    seeds = jax.random.split(jax.random.key(seed), 6)
    part_keys = jax.random.split(jax.random.fold_in(seeds[5], part), 6)
    return {
        "tracers": noise(part_keys[0], (LEV, NY, NX, C), 1.0, 6.0, ((1, 4), (2, 4)), jnp.float32),
        "adjoint_in": noise(part_keys[1], (LEV, NY, NX, C), 1.0, 6.0, ((1, 4), (2, 4)), jnp.float32),
        "shifts": draw_shifts(jax.random.fold_in(seeds[5], 71), part),
        "fractions": jnp.clip(jax.random.uniform(seeds[3], (LEV, NY), jnp.float32, 0.05, 0.95), 0.05, 0.95),
        "meridional": jnp.clip(jax.random.uniform(seeds[4], (LEV, NY, NX), jnp.float32, -0.9, 0.9) * steps_of(seeds[4], (LEV, NY, NX), ((2, 4),), -0.4, 0.0), -0.9, 0.9),
    }


def take_slice(values_in, start_at, stop_at, dimension):
    return lax.slice_in_dim(values_in, start_at, stop_at, axis=dimension)

def edge_values(values_in, amount, dimension):
    inner_sum = take_slice(values_in, 1, amount + 1, dimension) + take_slice(values_in, 2, amount + 2, dimension)
    outer_sum = take_slice(values_in, 0, amount, dimension) + take_slice(values_in, 3, amount + 3, dimension)
    return (7.0 * inner_sum - outer_sum) / 12.0

def cell_profile(values_in, dimension):
    interior = values_in.shape[dimension] - 6
    edge_row = edge_values(values_in, interior + 3, dimension)
    left_edge = take_slice(edge_row, 0, interior + 2, dimension)
    right_edge = take_slice(edge_row, 1, interior + 3, dimension)
    centres = take_slice(values_in, 2, interior + 4, dimension)
    curvature = 6.0 * centres - 3.0 * (left_edge + right_edge)
    return (interior, left_edge, right_edge, right_edge - left_edge, curvature)

def zonal_step(values_in, courant, dimension):
    interior, left_edge, right_edge, difference, curvature = cell_profile(values_in, dimension)
    transport = courant * (right_edge - 0.5 * courant * (difference - (1.0 - courant * (2.0 / 3.0)) * curvature))
    return take_slice(values_in, 3, interior + 3, dimension) - take_slice(transport, 1, interior + 1, dimension) + take_slice(transport, 0, interior, dimension)

def meridional_step(values_in, face_courant, dimension):
    interior, left_edge, right_edge, difference, curvature = cell_profile(values_in, dimension)

    def below_part(source):
        return take_slice(source, 0, interior + 1, dimension)

    def above_part(source):
        return take_slice(source, 1, interior + 2, dimension)
    northward = face_courant * (below_part(right_edge) - 0.5 * face_courant * (below_part(difference) - (1.0 - face_courant * (2.0 / 3.0)) * below_part(curvature)))
    southward = face_courant * (above_part(left_edge) - 0.5 * face_courant * above_part(difference) - above_part(curvature) * (0.5 * face_courant + face_courant * face_courant / 3.0))
    transport = jnp.where(face_courant > 0.0, northward, southward)
    return take_slice(values_in, 3, interior + 3, dimension) - take_slice(transport, 1, interior + 1, dimension) + take_slice(transport, 0, interior, dimension)

def advect_level(values_in, shift_row, fraction_row, face_level):
    width_cells = values_in.shape[1]
    positions = jnp.mod(jnp.arange(width_cells, dtype=jnp.int32)[None, :] - shift_row[:, None].astype(jnp.int32), width_cells).astype(jnp.int32)
    shifted = jnp.take_along_axis(values_in, positions[:, :, None], axis=1)
    wrapped = jnp.concatenate([shifted[:, -3:], shifted, shifted[:, :3]], axis=1)
    zonal = zonal_step(wrapped, fraction_row[:, None, None], 1)
    padded = jnp.pad(zonal, ((3, 3), (0, 0), (0, 0)))
    return meridional_step(padded, face_level[:, :, None], 0)

def reference(tracers, adjoint_in, shifts, fractions, meridional):
    forward_levels = []
    backward_levels = []
    for level_index in range(LEV):
        zero_row = jnp.zeros((1, NX), meridional.dtype)
        face_level = jnp.concatenate([zero_row, meridional[level_index, 1:], zero_row], axis=0)

        def one_level(values_in):
            return advect_level(values_in, shifts[level_index], fractions[level_index], face_level)
        result, pullback = jax.vjp(one_level, tracers[level_index])
        forward_levels.append(result)
        backward_levels.append(pullback(adjoint_in[level_index])[0])
    return (jnp.stack(forward_levels), jnp.stack(backward_levels))
```

```python
import functools

import jax
import jax.numpy as jnp
from jax import lax
from jax.experimental import pallas as pl
from jax.experimental.pallas import tpu as pltpu
from jax.sharding import PartitionSpec as P

MESH = pl.DeviceIdType.MESH
SUB = 8
RIM = 3


def chunk_list(levels, rows, step):
    return [(lv, r0) for lv in range(levels) for r0 in range(0, rows, step)]


def face_terms(v):
    size = jnp.abs(v)
    beta = v * (0.5 * size) * (1.0 - size * (2.0 / 3.0))
    return beta, 0.5 * v * v


def zonal_taps(c):
    b = 1.0 - c * (2.0 / 3.0)
    p = c * (1.0 - 0.5 * c - 1.5 * c * b)
    q = c * (0.5 * c - 1.5 * c * b)
    r = 3.0 * c * c * b
    d = p - q
    t = 1.0 / 12.0
    s = 7.0 / 12.0
    return (
        -t * q,
        s * q - t * d,
        r + t * p + s * d + s * q,
        1.0 - r - s * p + s * d - t * q,
        -s * p - t * d,
        t * p,
    )


def kernel(dims, *refs):
    levels, rows, cells, width, n_lon, n_lat, step = dims
    chunks = chunk_list(levels, rows, step)
    nq = len(chunks)
    tr, ad, shifts, fractions, mer, out_f, out_a = refs[:7]
    gath = (refs[7 : 7 + nq], refs[7 + nq : 7 + 2 * nq])
    zb, ab, vb, taps, of, oa, loc, ssem, rsem, hs, hr, osem = refs[7 + 2 * nq :]
    total_cells = cells * n_lon
    total_rows = rows * n_lat
    n_x = n_lon // 2

    me = lax.axis_index("lon")
    lat = lax.axis_index("lat")
    first = lat * rows
    core = lax.rem(me, 2)
    partner = me + 1 - 2 * core

    own = []
    dup = []
    for q, (lv, r0) in enumerate(chunks):
        a = pltpu.make_async_copy(
            tr.at[lv, pl.ds(r0, step)], gath[0][q].at[:, pl.ds(0, cells)], loc.at[q]
        )
        a.start()
        own.append(a)
    adc = pltpu.make_async_copy(ad, ab.at[:, pl.ds(RIM, rows)], loc.at[2 * nq])
    adc.start()
    for q, (lv, r0) in enumerate(chunks):
        b = pltpu.make_async_copy(
            tr.at[lv, pl.ds(r0, step)],
            gath[0][q].at[:, pl.ds(total_cells, cells)],
            loc.at[nq + q],
        )
        b.start()
        dup.append(b)

    barrier = pltpu.get_barrier_semaphore()
    pl.semaphore_signal(barrier, inc=1, device_id={"lon": partner}, device_id_type=MESH)
    for dx in range(1, n_x):
        pl.semaphore_signal(
            barrier, inc=1, device_id={"lon": lax.rem(me + 2 * dx, n_lon)}, device_id_type=MESH
        )

    @pl.when(lat > 0)
    def _():
        pl.semaphore_signal(barrier, inc=1, device_id={"lat": lat - 1}, device_id_type=MESH)

    @pl.when(lat < n_lat - 1)
    def _():
        pl.semaphore_signal(barrier, inc=1, device_id={"lat": lat + 1}, device_id_type=MESH)

    inner = jnp.logical_and(lat > 0, lat < n_lat - 1)

    @pl.when(inner)
    def _():
        pl.semaphore_wait(barrier, n_x + 2)

    @pl.when(jnp.logical_not(inner))
    def _():
        pl.semaphore_wait(barrier, n_x + min(n_lat - 1, 1))

    def lat_copies(buf, k):
        down = pltpu.make_async_remote_copy(
            buf.at[:, pl.ds(RIM, RIM)],
            buf.at[:, pl.ds(RIM + rows, RIM)],
            hs.at[k, 0],
            hr.at[k, 0],
            device_id={"lat": lat - 1},
            device_id_type=MESH,
        )
        up = pltpu.make_async_remote_copy(
            buf.at[:, pl.ds(rows, RIM)],
            buf.at[:, pl.ds(0, RIM)],
            hs.at[k, 1],
            hr.at[k, 1],
            device_id={"lat": lat + 1},
            device_id_type=MESH,
        )
        return down, up

    def lat_start(buf, k):
        down, up = lat_copies(buf, k)

        @pl.when(lat > 0)
        def _():
            down.start()

        @pl.when(lat < n_lat - 1)
        def _():
            up.start()

    def lat_wait(buf, k):
        down, up = lat_copies(buf, k)

        @pl.when(lat > 0)
        def _():
            down.wait_send()
            up.wait_recv()

        @pl.when(lat < n_lat - 1)
        def _():
            up.wait_send()
            down.wait_recv()

    def x_copy(a, q, dx):
        return pltpu.make_async_remote_copy(
            gath[a][q].at[:, pl.ds(0, cells)],
            gath[a][q].at[:, pl.ds((n_lon - 2 * dx) * cells, cells)],
            ssem.at[a, q, dx],
            rsem.at[a, q, dx],
            device_id={"lon": lax.rem(me + 2 * dx, n_lon)},
            device_id_type=MESH,
        )

    def core_copy(a, q, dx):
        source = ((n_lon - 2 * dx) % n_lon) * cells
        slot = lax.rem(2 * n_lon - 2 * dx + 2 * core - 1, n_lon)
        return pltpu.make_async_remote_copy(
            gath[a][q].at[:, pl.ds(source, cells)],
            gath[a][q].at[:, pl.ds(pl.multiple_of(slot * cells, cells), cells)],
            ssem.at[a, q, n_x + dx],
            rsem.at[a, q, n_x + dx],
            device_id={"lon": partner},
            device_id_type=MESH,
        )

    def gather_start(a, q):
        for dx in range(1, n_x):
            x_copy(a, q, dx).start()
        core_copy(a, q, 0).start()

    def relay(a, q):
        for dx in range(1, n_x):
            x_copy(a, q, dx).wait_recv()
            core_copy(a, q, dx).start()

    def gather_finish(a, q):
        for dx in range(n_x):
            core_copy(a, q, dx).wait_recv()

    def gather_drain(a, q):
        for dx in range(1, n_x):
            x_copy(a, q, dx).wait_send()
        for dx in range(n_x):
            core_copy(a, q, dx).wait_send()

    adc.wait()
    lat_start(ab, 0)
    for q in range(nq):
        own[q].wait()
        gather_start(0, q)

    @pl.when(lat == 0)
    def _():
        for buf in (ab, zb):
            buf[:, pl.ds(0, RIM)] = jnp.zeros((levels, RIM, cells, width), jnp.float32)

    @pl.when(lat == n_lat - 1)
    def _():
        for buf in (ab, zb):
            buf[:, pl.ds(RIM + rows, RIM)] = jnp.zeros((levels, RIM, cells, width), jnp.float32)

    faces = rows + 5
    for lv in range(levels):

        @pl.loop(0, faces)
        def _(f):
            row = first + f - 2
            line = mer[lv, pl.ds(lax.rem(row + total_rows, total_rows), 1), :]
            tall = jnp.broadcast_to(line, (width, cells)).T
            inside = jnp.logical_and(row > 0, row < total_rows)
            vb[lv, f] = jnp.where(inside, tall, 0.0)

        @pl.loop(0, rows)
        def _(r):
            for k, t in enumerate(zonal_taps(fractions[lv, first + r])):
                taps[(lv * rows + r) * 6 + k] = t

    lat_wait(ab, 0)
    for lv in range(levels):

        @pl.loop(0, cells // SUB)
        def _(c):
            at = pl.ds(pl.multiple_of(c * SUB, SUB), SUB)
            ev, q6b, dqb, eb = {}, {}, {}, {}
            carry = None
            y = {r: ab[lv, r + RIM, at, :] for r in range(-3, -1)}
            for f in range(-2, rows + 3):
                y[f] = ab[lv, f + RIM, at, :]
                v = vb[lv, f + 2, at, :]
                north = v > 0.0
                beta, gamma = face_terms(v)
                change = y[f] - y[f - 1]
                ev[f] = v * change
                b = beta * change
                g = -gamma * change
                bn, gn = jnp.where(north, b, 0.0), jnp.where(north, g, 0.0)
                if carry is not None:
                    q6b[f - 1] = bn + carry[0]
                    dqb[f - 1] = gn + carry[1]
                carry = (b - bn, g - gn)
                h = f - 1
                if h >= -1:
                    eb[h] = ev[h] - 3.0 * (q6b[h - 1] + q6b[h]) + (dqb[h - 1] - dqb[h])
                r = h - 2
                if r >= 0:
                    value = (
                        y[r]
                        + 6.0 * q6b[r]
                        + (7.0 / 12.0) * (eb[r] + eb[r + 1])
                        - (1.0 / 12.0) * (eb[r - 1] + eb[r + 2])
                    )
                    q = lv * (rows // step) + r // step
                    gath[1][q][r % step, at, :] = value
                    gath[1][q][
                        r % step, pl.ds(pl.multiple_of(total_cells + c * SUB, SUB), SUB), :
                    ] = value

        for q, (l2, _r) in enumerate(chunks):
            if l2 == lv:
                gather_start(1, q)

    def sweep(a, q, sink, sink_row, sign):
        lv, r0 = chunks[q]
        buf = gath[a][q]

        @pl.loop(0, step)
        def _(r):
            buf[r, pl.ds(total_cells + cells, SUB), :] = buf[r, pl.ds(cells, SUB), :]
            shift = shifts[lv, first + r0 + r]
            if sign < 0:
                start = lax.rem(2 * total_cells - shift - 3, total_cells)
            else:
                start = lax.rem(2 * total_cells + shift - 2, total_cells)
            base = (lv * rows + r0 + r) * 6
            w = [taps[base + k] for k in range(6)]
            if sign > 0:
                w = w[::-1]
            for c in range(cells // SUB):
                total = None
                for k in range(6):
                    term = w[k] * buf[r, pl.ds(start + c * SUB + k, SUB), :]
                    total = term if total is None else total + term
                sink[lv, sink_row + r0 + r, pl.ds(c * SUB, SUB), :] = total

    for b in dup:
        b.wait()
    for q in range(nq):
        relay(0, q)
        if q > 0:
            gather_finish(0, q - 1)
            sweep(0, q - 1, zb, RIM, -1)
    gather_finish(0, nq - 1)
    sweep(0, nq - 1, zb, RIM, -1)
    lat_start(zb, 1)

    relay(1, 0)
    lat_wait(zb, 1)

    for lv in range(levels):

        @pl.loop(0, cells // SUB)
        def _(c):
            at = pl.ds(pl.multiple_of(c * SUB, SUB), SUB)
            z = {r: zb[lv, r + RIM, at, :] for r in range(-3, 0)}
            e, q6, dq, flux = {}, {}, {}, {}
            for f in range(-1, rows + 2):
                z[f + 1] = zb[lv, f + 1 + RIM, at, :]
                e[f] = (7.0 / 12.0) * (z[f - 1] + z[f]) - (1.0 / 12.0) * (z[f - 2] + z[f + 1])
                u = f - 1
                if u >= -1:
                    q6[u] = 6.0 * z[u] - 3.0 * (e[u] + e[f])
                    dq[u] = e[f] - e[u]
                if u >= 0:
                    v = vb[lv, u + 2, at, :]
                    north = v > 0.0
                    beta, gamma = face_terms(v)
                    flux[u] = (
                        v * e[u]
                        + beta * jnp.where(north, q6[u - 1], q6[u])
                        - gamma * jnp.where(north, dq[u - 1], dq[u])
                    )
                if u >= 1:
                    of[lv, u - 1, at, :] = z[u - 1] - flux[u] + flux[u - 1]

    store_f = pltpu.make_async_copy(of, out_f, osem.at[nq])
    store_f.start()

    stores = []

    def finish_adjoint(q):
        lv, r0 = chunks[q]
        gather_finish(1, q)
        sweep(1, q, oa, 0, 1)
        s = pltpu.make_async_copy(
            oa.at[lv, pl.ds(r0, step)], out_a.at[lv, pl.ds(r0, step)], osem.at[q]
        )
        s.start()
        stores.append(s)

    for q in range(1, nq):
        relay(1, q)
        finish_adjoint(q - 1)
    finish_adjoint(nq - 1)

    for a in range(2):
        for q in range(nq):
            gather_drain(a, q)
    store_f.wait()
    for s in stores:
        s.wait()


def local(tracers, adjoint_in, shifts, fractions, meridional):
    levels, rows, cells, width = tracers.shape
    n_lon, n_lat = lax.axis_size("lon"), lax.axis_size("lat")
    step = max(1, rows // 4)
    nq = levels * (rows // step)
    n_x = n_lon // 2
    dims = (levels, rows, cells, width, n_lon, n_lat, step)
    block = pltpu.VMEM((step, (n_lon + 1) * cells + SUB, width), jnp.float32)
    banded = pltpu.VMEM((levels, rows + 2 * RIM, cells, width), jnp.float32)
    whole = pltpu.VMEM((levels, rows, cells, width), jnp.float32)
    anywhere = pl.BlockSpec(memory_space=pl.ANY)
    scalar = pl.BlockSpec(memory_space=pltpu.SMEM)
    shape = jax.ShapeDtypeStruct(tracers.shape, jnp.float32)
    return pl.pallas_call(
        functools.partial(kernel, dims),
        out_shape=(shape, shape),
        in_specs=[anywhere, anywhere, scalar, scalar, pl.BlockSpec(memory_space=pltpu.VMEM)],
        out_specs=(anywhere, anywhere),
        scratch_shapes=[block] * (2 * nq)
        + [
            banded,
            banded,
            pltpu.VMEM((levels, rows + 5, cells, width), jnp.float32),
            pltpu.SMEM((levels * rows * 6,), jnp.float32),
            whole,
            whole,
            pltpu.SemaphoreType.DMA((2 * nq + 1,)),
            pltpu.SemaphoreType.DMA((2, nq, 2 * n_x)),
            pltpu.SemaphoreType.DMA((2, nq, 2 * n_x)),
            pltpu.SemaphoreType.DMA((2, 2)),
            pltpu.SemaphoreType.DMA((2, 2)),
            pltpu.SemaphoreType.DMA((nq + 1,)),
        ],
        compiler_params=pltpu.CompilerParams(
            collective_id=0, has_side_effects=True, vmem_limit_bytes=60 * 1024 * 1024
        ),
    )(tracers, adjoint_in, shifts, fractions, meridional)


def solution(mesh):
    block = P("grp", "lat", "lon", None)
    in_specs = (block, block, P(), P(), P(None, None, "lon"))
    return jax.shard_map(
        local, mesh=mesh, in_specs=in_specs, out_specs=(block, block), check_vma=False
    )
```

```python
import functools

import jax
import jax.numpy as jnp
from jax import lax
from jax.experimental import pallas as pl
from jax.experimental.pallas import tpu as pltpu
from jax.sharding import PartitionSpec as P

MESH = pl.DeviceIdType.MESH
SUB = 8
RIM = 3


def chunk_list(levels, rows, step):
    return [(lv, r0) for lv in range(levels) for r0 in range(0, rows, step)]


def face_terms(v):
    size = jnp.abs(v)
    beta = v * (0.5 * size) * (1.0 - size * (2.0 / 3.0))
    return beta, 0.5 * v * v


def zonal_taps(c):
    b = 1.0 - c * (2.0 / 3.0)
    p = c * (1.0 - 0.5 * c - 1.5 * c * b)
    q = c * (0.5 * c - 1.5 * c * b)
    r = 3.0 * c * c * b
    d = p - q
    t = 1.0 / 12.0
    s = 7.0 / 12.0
    return (
        -t * q,
        s * q - t * d,
        r + t * p + s * d + s * q,
        1.0 - r - s * p + s * d - t * q,
        -s * p - t * d,
        t * p,
    )


def kernel(dims, *refs):
    levels, rows, cells, width, n_lon, n_lat, step = dims
    chunks = chunk_list(levels, rows, step)
    nq = len(chunks)
    tr, ad, shifts_in, fractions_in, mer_in, of, oa = refs[:7]
    gath = (refs[7 : 7 + nq], refs[7 + nq : 7 + 2 * nq])
    zb, ab, vb, taps, shifts, fractions, mer, loc, ssem, rsem, hs, hr = refs[7 + 2 * nq :]
    total_cells = cells * n_lon
    total_rows = rows * n_lat
    n_x = n_lon // 2

    me = lax.axis_index("lon")
    lat = lax.axis_index("lat")
    first = lat * rows
    core = lax.rem(me, 2)
    partner = me + 1 - 2 * core

    own = []
    dup = []
    for q, (lv, r0) in enumerate(chunks):
        a = pltpu.make_async_copy(
            tr.at[lv, pl.ds(r0, step)], gath[0][q].at[:, pl.ds(0, cells)], loc.at[q]
        )
        a.start()
        own.append(a)
    adc = pltpu.make_async_copy(ad, ab.at[:, pl.ds(RIM, rows)], loc.at[2 * nq])
    adc.start()
    for q, (lv, r0) in enumerate(chunks):
        b = pltpu.make_async_copy(
            tr.at[lv, pl.ds(r0, step)],
            gath[0][q].at[:, pl.ds(total_cells, cells)],
            loc.at[nq + q],
        )
        b.start()
        dup.append(b)

    small = []
    for k, (source, target) in enumerate(
        ((shifts_in, shifts), (fractions_in, fractions), (mer_in, mer))
    ):
        d = pltpu.make_async_copy(source, target, loc.at[2 * nq + 1 + k])
        d.start()
        small.append(d)

    barrier = pltpu.get_barrier_semaphore()
    pl.semaphore_signal(barrier, inc=1, device_id={"lon": partner}, device_id_type=MESH)
    for dx in range(1, n_x):
        pl.semaphore_signal(
            barrier, inc=1, device_id={"lon": lax.rem(me + 2 * dx, n_lon)}, device_id_type=MESH
        )

    @pl.when(lat > 0)
    def _():
        pl.semaphore_signal(barrier, inc=1, device_id={"lat": lat - 1}, device_id_type=MESH)

    @pl.when(lat < n_lat - 1)
    def _():
        pl.semaphore_signal(barrier, inc=1, device_id={"lat": lat + 1}, device_id_type=MESH)

    inner = jnp.logical_and(lat > 0, lat < n_lat - 1)

    @pl.when(inner)
    def _():
        pl.semaphore_wait(barrier, n_x + 2)

    @pl.when(jnp.logical_not(inner))
    def _():
        pl.semaphore_wait(barrier, n_x + min(n_lat - 1, 1))

    def lat_copies(buf, k):
        down = pltpu.make_async_remote_copy(
            buf.at[:, pl.ds(RIM, RIM)],
            buf.at[:, pl.ds(RIM + rows, RIM)],
            hs.at[k, 0],
            hr.at[k, 0],
            device_id={"lat": lat - 1},
            device_id_type=MESH,
        )
        up = pltpu.make_async_remote_copy(
            buf.at[:, pl.ds(rows, RIM)],
            buf.at[:, pl.ds(0, RIM)],
            hs.at[k, 1],
            hr.at[k, 1],
            device_id={"lat": lat + 1},
            device_id_type=MESH,
        )
        return down, up

    def lat_start(buf, k):
        down, up = lat_copies(buf, k)

        @pl.when(lat > 0)
        def _():
            down.start()

        @pl.when(lat < n_lat - 1)
        def _():
            up.start()

    def lat_wait(buf, k):
        down, up = lat_copies(buf, k)

        @pl.when(lat > 0)
        def _():
            down.wait_send()
            up.wait_recv()

        @pl.when(lat < n_lat - 1)
        def _():
            up.wait_send()
            down.wait_recv()

    def x_copy(a, q, dx):
        return pltpu.make_async_remote_copy(
            gath[a][q].at[:, pl.ds(0, cells)],
            gath[a][q].at[:, pl.ds((n_lon - 2 * dx) * cells, cells)],
            ssem.at[a, q, dx],
            rsem.at[a, q, dx],
            device_id={"lon": lax.rem(me + 2 * dx, n_lon)},
            device_id_type=MESH,
        )

    def core_copy(a, q, dx):
        source = ((n_lon - 2 * dx) % n_lon) * cells
        slot = lax.rem(2 * n_lon - 2 * dx + 2 * core - 1, n_lon)
        return pltpu.make_async_remote_copy(
            gath[a][q].at[:, pl.ds(source, cells)],
            gath[a][q].at[:, pl.ds(pl.multiple_of(slot * cells, cells), cells)],
            ssem.at[a, q, n_x + dx],
            rsem.at[a, q, n_x + dx],
            device_id={"lon": partner},
            device_id_type=MESH,
        )

    def gather_start(a, q):
        for dx in range(1, n_x):
            x_copy(a, q, dx).start()
        core_copy(a, q, 0).start()

    def relay(a, q):
        for dx in range(1, n_x):
            x_copy(a, q, dx).wait_recv()
            core_copy(a, q, dx).start()

    def gather_finish(a, q):
        for dx in range(n_x):
            core_copy(a, q, dx).wait_recv()

    def gather_drain(a, q):
        for dx in range(1, n_x):
            x_copy(a, q, dx).wait_send()
        for dx in range(n_x):
            core_copy(a, q, dx).wait_send()

    adc.wait()
    lat_start(ab, 0)
    for q in range(nq):
        own[q].wait()
        gather_start(0, q)

    @pl.when(lat == 0)
    def _():
        for buf in (ab, zb):
            buf[:, pl.ds(0, RIM)] = jnp.zeros((levels, RIM, cells, width), jnp.float32)

    @pl.when(lat == n_lat - 1)
    def _():
        for buf in (ab, zb):
            buf[:, pl.ds(RIM + rows, RIM)] = jnp.zeros((levels, RIM, cells, width), jnp.float32)

    for d in small:
        d.wait()
    faces = rows + 5
    lanes = lax.broadcasted_iota(jnp.int32, (cells, total_rows), 1)
    for lv in range(levels):

        @pl.loop(0, faces)
        def _(f):
            row = first + f - 2
            chosen = jnp.logical_and(lanes == row, lanes > 0)
            column = jnp.sum(jnp.where(chosen, mer[lv], 0.0), axis=1, keepdims=True)
            vb[lv, f] = jnp.broadcast_to(column, (cells, width))

        @pl.loop(0, rows)
        def _(r):
            for k, t in enumerate(zonal_taps(fractions[lv, first + r])):
                taps[(lv * rows + r) * 6 + k] = t

    lat_wait(ab, 0)
    for lv in range(levels):

        @pl.loop(0, cells // SUB)
        def _(c):
            at = pl.ds(pl.multiple_of(c * SUB, SUB), SUB)
            ev, q6b, dqb, eb = {}, {}, {}, {}
            carry = None
            y = {r: ab[lv, r + RIM, at, :] for r in range(-3, -1)}
            for f in range(-2, rows + 3):
                y[f] = ab[lv, f + RIM, at, :]
                v = vb[lv, f + 2, at, :]
                north = v > 0.0
                beta, gamma = face_terms(v)
                change = y[f] - y[f - 1]
                ev[f] = v * change
                b = beta * change
                g = -gamma * change
                bn, gn = jnp.where(north, b, 0.0), jnp.where(north, g, 0.0)
                if carry is not None:
                    q6b[f - 1] = bn + carry[0]
                    dqb[f - 1] = gn + carry[1]
                carry = (b - bn, g - gn)
                h = f - 1
                if h >= -1:
                    eb[h] = ev[h] - 3.0 * (q6b[h - 1] + q6b[h]) + (dqb[h - 1] - dqb[h])
                r = h - 2
                if r >= 0:
                    value = (
                        y[r]
                        + 6.0 * q6b[r]
                        + (7.0 / 12.0) * (eb[r] + eb[r + 1])
                        - (1.0 / 12.0) * (eb[r - 1] + eb[r + 2])
                    )
                    q = lv * (rows // step) + r // step
                    gath[1][q][r % step, at, :] = value
                    gath[1][q][
                        r % step, pl.ds(pl.multiple_of(total_cells + c * SUB, SUB), SUB), :
                    ] = value

        for q, (l2, _r) in enumerate(chunks):
            if l2 == lv:
                gather_start(1, q)

    def sweep(a, q, sink, sink_row, sign):
        lv, r0 = chunks[q]
        buf = gath[a][q]

        @pl.loop(0, step)
        def _(r):
            buf[r, pl.ds(total_cells + cells, SUB), :] = buf[r, pl.ds(cells, SUB), :]
            shift = shifts[lv, first + r0 + r]
            if sign < 0:
                start = lax.rem(2 * total_cells - shift - 3, total_cells)
            else:
                start = lax.rem(2 * total_cells + shift - 2, total_cells)
            base = (lv * rows + r0 + r) * 6
            w = [taps[base + k] for k in range(6)]
            if sign > 0:
                w = w[::-1]
            for c in range(cells // SUB):
                total = None
                for k in range(6):
                    term = w[k] * buf[r, pl.ds(start + c * SUB + k, SUB), :]
                    total = term if total is None else total + term
                sink[lv, sink_row + r0 + r, pl.ds(c * SUB, SUB), :] = total

    for b in dup:
        b.wait()
    for q in range(nq):
        relay(0, q)
        if q > 0:
            gather_finish(0, q - 1)
            sweep(0, q - 1, zb, RIM, -1)
    gather_finish(0, nq - 1)
    sweep(0, nq - 1, zb, RIM, -1)
    lat_start(zb, 1)

    relay(1, 0)
    lat_wait(zb, 1)

    for lv in range(levels):

        @pl.loop(0, cells // SUB)
        def _(c):
            at = pl.ds(pl.multiple_of(c * SUB, SUB), SUB)
            z = {r: zb[lv, r + RIM, at, :] for r in range(-3, 0)}
            e, q6, dq, flux = {}, {}, {}, {}
            for f in range(-1, rows + 2):
                z[f + 1] = zb[lv, f + 1 + RIM, at, :]
                e[f] = (7.0 / 12.0) * (z[f - 1] + z[f]) - (1.0 / 12.0) * (z[f - 2] + z[f + 1])
                u = f - 1
                if u >= -1:
                    q6[u] = 6.0 * z[u] - 3.0 * (e[u] + e[f])
                    dq[u] = e[f] - e[u]
                if u >= 0:
                    v = vb[lv, u + 2, at, :]
                    north = v > 0.0
                    beta, gamma = face_terms(v)
                    flux[u] = (
                        v * e[u]
                        + beta * jnp.where(north, q6[u - 1], q6[u])
                        - gamma * jnp.where(north, dq[u - 1], dq[u])
                    )
                if u >= 1:
                    of[lv, u - 1, at, :] = z[u - 1] - flux[u] + flux[u - 1]

    def finish_adjoint(q):
        lv, r0 = chunks[q]
        gather_finish(1, q)
        sweep(1, q, oa, 0, 1)

    for q in range(1, nq):
        relay(1, q)
        finish_adjoint(q - 1)
    finish_adjoint(nq - 1)

    for a in range(2):
        for q in range(nq):
            gather_drain(a, q)


def local(tracers, adjoint_in, shifts, fractions, meridional):
    levels, rows, cells, width = tracers.shape
    n_lon, n_lat = lax.axis_size("lon"), lax.axis_size("lat")
    step = max(1, rows // 4)
    nq = levels * (rows // step)
    n_x = n_lon // 2
    dims = (levels, rows, cells, width, n_lon, n_lat, step)
    block = pltpu.VMEM((step, (n_lon + 1) * cells + SUB, width), jnp.float32)
    banded = pltpu.VMEM((levels, rows + 2 * RIM, cells, width), jnp.float32)
    vmem = pl.BlockSpec(memory_space=pltpu.VMEM)
    held = 2 * levels * rows * ((n_lon + 1) * cells + SUB) + levels * (5 * rows + 17) * cells
    far = pl.BlockSpec(memory_space=pltpu.HBM)
    shape = jax.ShapeDtypeStruct(tracers.shape, jnp.float32)
    return pl.pallas_call(
        functools.partial(kernel, dims),
        out_shape=(shape, shape),
        in_specs=[far] * 5,
        out_specs=(vmem, vmem),
        scratch_shapes=[block] * (2 * nq)
        + [
            banded,
            banded,
            pltpu.VMEM((levels, rows + 5, cells, width), jnp.float32),
            pltpu.SMEM((levels * rows * 6,), jnp.float32),
            pltpu.SMEM(shifts.shape, jnp.int32),
            pltpu.SMEM(fractions.shape, jnp.float32),
            pltpu.VMEM((levels, cells, meridional.shape[1]), jnp.float32),
            pltpu.SemaphoreType.DMA((2 * nq + 4,)),
            pltpu.SemaphoreType.DMA((2, nq, 2 * n_x)),
            pltpu.SemaphoreType.DMA((2, nq, 2 * n_x)),
            pltpu.SemaphoreType.DMA((2, 2)),
            pltpu.SemaphoreType.DMA((2, 2)),
        ],
        compiler_params=pltpu.CompilerParams(
            collective_id=0, has_side_effects=True, vmem_limit_bytes=held * width * 4 + (6 << 20)
        ),
    )(tracers, adjoint_in, shifts, fractions, jnp.swapaxes(meridional, 1, 2))


def solution(mesh):
    block = P("grp", "lat", "lon", None)
    in_specs = (block, block, P(), P(), P(None, None, "lon"))
    return jax.shard_map(
        local, mesh=mesh, in_specs=in_specs, out_specs=(block, block), check_vma=False
    )
```

```python
import functools

import jax
import jax.numpy as jnp
from jax import lax
from jax.experimental import pallas as pl
from jax.experimental.pallas import tpu as pltpu
from jax.sharding import PartitionSpec as P

MESH = pl.DeviceIdType.MESH
SUB = 8
RIM = 3
ROUTE = 0


def chunk_list(levels, rows, step):
    return [(lv, r0) for lv in range(levels) for r0 in range(0, rows, step)]


def reach(total_cells, total_rows, row):
    d = abs(2 * row + 1 - total_rows)
    return (total_cells - 1) * d * d // ((total_rows - 1) * (total_rows - 1))


def span_of(dims, a, r0, lat, core):
    levels, rows, cells, width, n_lon, n_lat, step = dims
    if n_lon != 4:
        return (0, cells)
    most = max(
        reach(cells * n_lon, rows * n_lat, lat * rows + r) for r in range(r0, r0 + step)
    )
    if most + 4 > cells:
        return (0, cells)
    long = -(-(most + RIM) // SUB) * SUB
    if a == 0:
        return (cells - long, cells) if core else (0, SUB)
    return (cells - SUB, cells) if core else (0, long)


def face_terms(v):
    size = jnp.abs(v)
    beta = v * (0.5 * size) * (1.0 - size * (2.0 / 3.0))
    return beta, 0.5 * v * v


def zonal_taps(c):
    b = 1.0 - c * (2.0 / 3.0)
    p = c * (1.0 - 0.5 * c - 1.5 * c * b)
    q = c * (0.5 * c - 1.5 * c * b)
    r = 3.0 * c * c * b
    d = p - q
    t = 1.0 / 12.0
    s = 7.0 / 12.0
    return (
        -t * q,
        s * q - t * d,
        r + t * p + s * d + s * q,
        1.0 - r - s * p + s * d - t * q,
        -s * p - t * d,
        t * p,
    )


def kernel(dims, *refs):
    levels, rows, cells, width, n_lon, n_lat, step = dims
    chunks = chunk_list(levels, rows, step)
    nq = len(chunks)
    tr, ad, shifts_in, fractions_in, mer_in, of, oa = refs[:7]
    gath = (refs[7 : 7 + nq], refs[7 + nq : 7 + 2 * nq])
    zb, ab, vb, taps, shifts, fractions, mer, held, loc, ssem, rsem, hs, hr, vs, vr = refs[7 + 2 * nq :]
    total_cells = cells * n_lon
    total_rows = rows * n_lat
    n_x = n_lon // 2

    me = lax.axis_index("lon")
    lat = lax.axis_index("lat")
    first = lat * rows
    core = lax.rem(me, 2)
    partner = me + 1 - 2 * core
    via = n_lon == 4 and n_lat == 4 and nq >= 4
    half = nq // 2
    detour = [half - 2, half - 1] if via else []
    if via:
        order = list(range(half - 2)) + list(range(half, nq - 2)) + detour + [nq - 2, nq - 1]
    else:
        order = list(range(nq))
    mate = lat + 1 - 2 * lax.rem(lat, 2)
    across = {"lon": lax.rem(me + 2, n_lon), "lat": mate}
    helper = jnp.logical_and(lat > 0, lat < n_lat - 1)
    helped = jnp.logical_not(helper)

    own = []
    dup = []
    for q, (lv, r0) in enumerate(chunks):
        a = pltpu.make_async_copy(
            tr.at[lv, pl.ds(r0, step)], gath[0][q].at[:, pl.ds(0, cells)], loc.at[q]
        )
        a.start()
        own.append(a)
    adc = pltpu.make_async_copy(ad, ab.at[:, pl.ds(RIM, rows)], loc.at[2 * nq])
    adc.start()
    for q, (lv, r0) in enumerate(chunks):
        b = pltpu.make_async_copy(
            tr.at[lv, pl.ds(r0, step)],
            gath[0][q].at[:, pl.ds(total_cells, cells)],
            loc.at[nq + q],
        )
        b.start()
        dup.append(b)

    small = []
    for k, (source, target) in enumerate(
        ((shifts_in, shifts), (fractions_in, fractions), (mer_in, mer))
    ):
        d = pltpu.make_async_copy(source, target, loc.at[2 * nq + 1 + k])
        d.start()
        small.append(d)

    barrier = pltpu.get_barrier_semaphore()
    pl.semaphore_signal(barrier, inc=1, device_id={"lon": partner}, device_id_type=MESH)
    for dx in range(1, n_x):
        pl.semaphore_signal(
            barrier, inc=1, device_id={"lon": lax.rem(me + 2 * dx, n_lon)}, device_id_type=MESH
        )

    if via:
        pl.semaphore_signal(barrier, inc=1, device_id=across, device_id_type=MESH)

    @pl.when(lat > 0)
    def _():
        pl.semaphore_signal(barrier, inc=1, device_id={"lat": lat - 1}, device_id_type=MESH)

    @pl.when(lat < n_lat - 1)
    def _():
        pl.semaphore_signal(barrier, inc=1, device_id={"lat": lat + 1}, device_id_type=MESH)

    inner = jnp.logical_and(lat > 0, lat < n_lat - 1)

    @pl.when(inner)
    def _():
        pl.semaphore_wait(barrier, n_x + 2 + int(via))

    @pl.when(jnp.logical_not(inner))
    def _():
        pl.semaphore_wait(barrier, n_x + min(n_lat - 1, 1) + int(via))

    def lat_copies(buf, k):
        down = pltpu.make_async_remote_copy(
            buf.at[:, pl.ds(RIM, RIM)],
            buf.at[:, pl.ds(RIM + rows, RIM)],
            hs.at[k, 0],
            hr.at[k, 0],
            device_id={"lat": lat - 1},
            device_id_type=MESH,
        )
        up = pltpu.make_async_remote_copy(
            buf.at[:, pl.ds(rows, RIM)],
            buf.at[:, pl.ds(0, RIM)],
            hs.at[k, 1],
            hr.at[k, 1],
            device_id={"lat": lat + 1},
            device_id_type=MESH,
        )
        return down, up

    def lat_start(buf, k):
        down, up = lat_copies(buf, k)

        @pl.when(lat > 0)
        def _():
            down.start()

        @pl.when(lat < n_lat - 1)
        def _():
            up.start()

    def lat_wait(buf, k):
        down, up = lat_copies(buf, k)

        @pl.when(lat > 0)
        def _():
            down.wait_send()
            up.wait_recv()

        @pl.when(lat < n_lat - 1)
        def _():
            up.wait_send()
            down.wait_recv()

    def x_copy(a, q, dx, span):
        lo, hi = span
        return pltpu.make_async_remote_copy(
            gath[a][q].at[:, pl.ds(lo, hi - lo)],
            gath[a][q].at[:, pl.ds((n_lon - 2 * dx) * cells + lo, hi - lo)],
            ssem.at[a, q, dx],
            rsem.at[a, q, dx],
            device_id={"lon": lax.rem(me + 2 * dx, n_lon)},
            device_id_type=MESH,
        )

    def core_copy(a, q, dx, span):
        lo, hi = span
        source = ((n_lon - 2 * dx) % n_lon) * cells + lo
        slot = lax.rem(2 * n_lon - 2 * dx + 2 * core - 1, n_lon)
        return pltpu.make_async_remote_copy(
            gath[a][q].at[:, pl.ds(source, hi - lo)],
            gath[a][q].at[:, pl.ds(pl.multiple_of(slot * cells + lo, SUB), hi - lo)],
            ssem.at[a, q, n_x + dx],
            rsem.at[a, q, n_x + dx],
            device_id={"lon": partner},
            device_id_type=MESH,
        )

    def out_copy(a, q):
        i = detour.index(q)
        return pltpu.make_async_remote_copy(
            gath[a][q].at[:, pl.ds(0, cells)],
            held.at[a, i],
            vs.at[a, i, 0],
            vr.at[a, i, 0],
            device_id=across if ROUTE else {"lat": mate},
            device_id_type=MESH,
        )

    def on_copy(a, q):
        i = detour.index(q)
        return pltpu.make_async_remote_copy(
            held.at[a, i],
            gath[a][q].at[:, pl.ds((n_lon - 2) * cells, cells)],
            vs.at[a, i, 1],
            vr.at[a, i, 1],
            device_id={"lat": mate} if ROUTE else across,
            device_id_type=MESH,
        )

    whole = (0, cells)

    def by_span(a, q, who, act):
        groups = {}
        for z in range(n_lat):
            for k in range(2):
                groups.setdefault(span_of(dims, a, chunks[q][1], z, k), []).append((z, k))
        if len(groups) == 1:
            act(next(iter(groups)))
            return
        for span, places in groups.items():
            hit = None
            for z in range(n_lat):
                ks = [k for y, k in places if y == z]
                if not ks:
                    continue
                here = lat == z
                if len(ks) == 1:
                    here = jnp.logical_and(here, who == ks[0])
                hit = here if hit is None else jnp.logical_or(hit, here)

            @pl.when(hit)
            def _():
                act(span)

    def direct(a, q, act):
        if q in detour:

            @pl.when(helper)
            def _():
                by_span(a, q, core, act)

        else:
            by_span(a, q, core, act)

    def detoured(q, act):
        if q in detour:

            @pl.when(helped)
            def _():
                act()

    def gather_start(a, q):
        detoured(q, lambda: out_copy(a, q).start())
        for dx in range(1, n_x):
            direct(a, q, lambda span: x_copy(a, q, dx, span).start())
        core_copy(a, q, 0, whole).start()

    def pass_on(a):
        for q in detour:

            @pl.when(helper)
            def _():
                out_copy(a, q).wait_recv()
                on_copy(a, q).start()

    def relay(a, q):
        def ready():
            on_copy(a, q).wait_recv()
            core_copy(a, q, 1, whole).start()

        detoured(q, ready)
        for dx in range(1, n_x):

            def act(span):
                x_copy(a, q, dx, span).wait_recv()
                core_copy(a, q, dx, span).start()

            direct(a, q, act)

    def gather_finish(a, q):
        core_copy(a, q, 0, whole).wait_recv()
        for dx in range(1, n_x):
            by_span(a, q, 1 - core, lambda span: core_copy(a, q, dx, span).wait_recv())

    def gather_drain(a, q):
        detoured(q, lambda: out_copy(a, q).wait_send())
        if q in detour:

            @pl.when(helper)
            def _():
                on_copy(a, q).wait_send()

        core_copy(a, q, 0, whole).wait_send()
        for dx in range(1, n_x):
            direct(a, q, lambda span: x_copy(a, q, dx, span).wait_send())
            by_span(a, q, core, lambda span: core_copy(a, q, dx, span).wait_send())

    adc.wait()
    lat_start(ab, 0)
    for q in range(nq):
        own[q].wait()
        gather_start(0, q)

    @pl.when(lat == 0)
    def _():
        for buf in (ab, zb):
            buf[:, pl.ds(0, RIM)] = jnp.zeros((levels, RIM, cells, width), jnp.float32)

    @pl.when(lat == n_lat - 1)
    def _():
        for buf in (ab, zb):
            buf[:, pl.ds(RIM + rows, RIM)] = jnp.zeros((levels, RIM, cells, width), jnp.float32)

    for d in small:
        d.wait()
    faces = rows + 5
    lanes = lax.broadcasted_iota(jnp.int32, (cells, total_rows), 1)
    for lv in range(levels):

        @pl.loop(0, faces)
        def _(f):
            row = first + f - 2
            chosen = jnp.logical_and(lanes == row, lanes > 0)
            column = jnp.sum(jnp.where(chosen, mer[lv], 0.0), axis=1, keepdims=True)
            vb[lv, f] = jnp.broadcast_to(column, (cells, width))

        @pl.loop(0, rows)
        def _(r):
            for k, t in enumerate(zonal_taps(fractions[lv, first + r])):
                taps[(lv * rows + r) * 6 + k] = t

    pass_on(0)

    lat_wait(ab, 0)
    for lv in range(levels):

        @pl.loop(0, cells // SUB)
        def _(c):
            at = pl.ds(pl.multiple_of(c * SUB, SUB), SUB)
            ev, q6b, dqb, eb = {}, {}, {}, {}
            carry = None
            y = {r: ab[lv, r + RIM, at, :] for r in range(-3, -1)}
            for f in range(-2, rows + 3):
                y[f] = ab[lv, f + RIM, at, :]
                v = vb[lv, f + 2, at, :]
                north = v > 0.0
                beta, gamma = face_terms(v)
                change = y[f] - y[f - 1]
                ev[f] = v * change
                b = beta * change
                g = -gamma * change
                bn, gn = jnp.where(north, b, 0.0), jnp.where(north, g, 0.0)
                if carry is not None:
                    q6b[f - 1] = bn + carry[0]
                    dqb[f - 1] = gn + carry[1]
                carry = (b - bn, g - gn)
                h = f - 1
                if h >= -1:
                    eb[h] = ev[h] - 3.0 * (q6b[h - 1] + q6b[h]) + (dqb[h - 1] - dqb[h])
                r = h - 2
                if r >= 0:
                    value = (
                        y[r]
                        + 6.0 * q6b[r]
                        + (7.0 / 12.0) * (eb[r] + eb[r + 1])
                        - (1.0 / 12.0) * (eb[r - 1] + eb[r + 2])
                    )
                    q = lv * (rows // step) + r // step
                    gath[1][q][r % step, at, :] = value
                    gath[1][q][
                        r % step, pl.ds(pl.multiple_of(total_cells + c * SUB, SUB), SUB), :
                    ] = value

        if lv == levels - 1:
            pass_on(1)
        for q, (l2, _r) in enumerate(chunks):
            if l2 == lv:
                gather_start(1, q)

    def sweep(a, q, sink, sink_row, sign):
        lv, r0 = chunks[q]
        buf = gath[a][q]

        @pl.loop(0, step)
        def _(r):
            buf[r, pl.ds(total_cells + cells, SUB), :] = buf[r, pl.ds(cells, SUB), :]
            shift = shifts[lv, first + r0 + r]
            if sign < 0:
                start = lax.rem(2 * total_cells - shift - 3, total_cells)
            else:
                start = lax.rem(2 * total_cells + shift - 2, total_cells)
            base = (lv * rows + r0 + r) * 6
            w = [taps[base + k] for k in range(6)]
            if sign > 0:
                w = w[::-1]
            for c in range(cells // SUB):
                total = None
                for k in range(6):
                    term = w[k] * buf[r, pl.ds(start + c * SUB + k, SUB), :]
                    total = term if total is None else total + term
                sink[lv, sink_row + r0 + r, pl.ds(c * SUB, SUB), :] = total

    for b in dup:
        b.wait()
    for i, q in enumerate(order):
        relay(0, q)
        if i > 0:
            gather_finish(0, order[i - 1])
            sweep(0, order[i - 1], zb, RIM, -1)
    gather_finish(0, order[-1])
    sweep(0, order[-1], zb, RIM, -1)
    lat_start(zb, 1)

    relay(1, order[0])
    lat_wait(zb, 1)

    for lv in range(levels):

        @pl.loop(0, cells // SUB)
        def _(c):
            at = pl.ds(pl.multiple_of(c * SUB, SUB), SUB)
            z = {r: zb[lv, r + RIM, at, :] for r in range(-3, 0)}
            e, q6, dq, flux = {}, {}, {}, {}
            for f in range(-1, rows + 2):
                z[f + 1] = zb[lv, f + 1 + RIM, at, :]
                e[f] = (7.0 / 12.0) * (z[f - 1] + z[f]) - (1.0 / 12.0) * (z[f - 2] + z[f + 1])
                u = f - 1
                if u >= -1:
                    q6[u] = 6.0 * z[u] - 3.0 * (e[u] + e[f])
                    dq[u] = e[f] - e[u]
                if u >= 0:
                    v = vb[lv, u + 2, at, :]
                    north = v > 0.0
                    beta, gamma = face_terms(v)
                    flux[u] = (
                        v * e[u]
                        + beta * jnp.where(north, q6[u - 1], q6[u])
                        - gamma * jnp.where(north, dq[u - 1], dq[u])
                    )
                if u >= 1:
                    of[lv, u - 1, at, :] = z[u - 1] - flux[u] + flux[u - 1]

    def finish_adjoint(q):
        lv, r0 = chunks[q]
        gather_finish(1, q)
        sweep(1, q, oa, 0, 1)

    for i in range(1, nq):
        relay(1, order[i])
        finish_adjoint(order[i - 1])
    finish_adjoint(order[-1])

    for a in range(2):
        for q in range(nq):
            gather_drain(a, q)


def local(tracers, adjoint_in, shifts, fractions, meridional):
    levels, rows, cells, width = tracers.shape
    n_lon, n_lat = lax.axis_size("lon"), lax.axis_size("lat")
    step = max(1, rows // 4)
    nq = levels * (rows // step)
    n_x = n_lon // 2
    dims = (levels, rows, cells, width, n_lon, n_lat, step)
    block = pltpu.VMEM((step, (n_lon + 1) * cells + SUB, width), jnp.float32)
    banded = pltpu.VMEM((levels, rows + 2 * RIM, cells, width), jnp.float32)
    vmem = pl.BlockSpec(memory_space=pltpu.VMEM)
    far = pl.BlockSpec(memory_space=pltpu.HBM)
    shape = jax.ShapeDtypeStruct(tracers.shape, jnp.float32)
    return pl.pallas_call(
        functools.partial(kernel, dims),
        out_shape=(shape, shape),
        in_specs=[far] * 5,
        out_specs=(vmem, vmem),
        scratch_shapes=[block] * (2 * nq)
        + [
            banded,
            banded,
            pltpu.VMEM((levels, rows + 5, cells, width), jnp.float32),
            pltpu.SMEM((levels * rows * 6,), jnp.float32),
            pltpu.SMEM(shifts.shape, jnp.int32),
            pltpu.SMEM(fractions.shape, jnp.float32),
            pltpu.VMEM((levels, cells, meridional.shape[1]), jnp.float32),
            pltpu.VMEM((2, 2, step, cells, width), jnp.float32),
            pltpu.SemaphoreType.DMA((2 * nq + 4,)),
            pltpu.SemaphoreType.DMA((2, nq, 2 * n_x)),
            pltpu.SemaphoreType.DMA((2, nq, 2 * n_x)),
            pltpu.SemaphoreType.DMA((2, 2)),
            pltpu.SemaphoreType.DMA((2, 2)),
            pltpu.SemaphoreType.DMA((2, 2, 2)),
            pltpu.SemaphoreType.DMA((2, 2, 2)),
        ],
        compiler_params=pltpu.CompilerParams(
            collective_id=0, has_side_effects=True, vmem_limit_bytes=60 << 20
        ),
    )(tracers, adjoint_in, shifts, fractions, jnp.swapaxes(meridional, 1, 2))


def solution(mesh):
    block = P("grp", "lat", "lon", None)
    in_specs = (block, block, P(), P(), P(None, None, "lon"))
    return jax.shard_map(
        local, mesh=mesh, in_specs=in_specs, out_specs=(block, block), check_vma=False
    )
```

```python
import functools

import jax
import jax.numpy as jnp
from jax import lax
from jax.experimental import pallas as pl
from jax.experimental.pallas import tpu as pltpu
from jax.sharding import PartitionSpec as P

MESH = pl.DeviceIdType.MESH
SUB = 8
RIM = 3
ROUTE = 0


def chunk_list(levels, rows, step):
    return [(lv, r0) for lv in range(levels) for r0 in range(0, rows, step)]


def reach(total_cells, total_rows, row):
    d = abs(2 * row + 1 - total_rows)
    return (total_cells - 1) * d * d // ((total_rows - 1) * (total_rows - 1))


def span_of(dims, a, r0, lat, core):
    levels, rows, cells, width, n_lon, n_lat, step = dims
    if n_lon != 4:
        return (0, cells)
    most = max(
        reach(cells * n_lon, rows * n_lat, lat * rows + r) for r in range(r0, r0 + step)
    )
    if most + 4 > cells:
        return (0, cells)
    long = -(-(most + RIM) // SUB) * SUB
    if a == 0:
        return (cells - long, cells) if core else (0, SUB)
    return (cells - SUB, cells) if core else (0, long)


def face_terms(v):
    size = jnp.abs(v)
    beta = v * (0.5 * size) * (1.0 - size * (2.0 / 3.0))
    return beta, 0.5 * v * v


def zonal_taps(c):
    b = 1.0 - c * (2.0 / 3.0)
    p = c * (1.0 - 0.5 * c - 1.5 * c * b)
    q = c * (0.5 * c - 1.5 * c * b)
    r = 3.0 * c * c * b
    d = p - q
    t = 1.0 / 12.0
    s = 7.0 / 12.0
    return (
        -t * q,
        s * q - t * d,
        r + t * p + s * d + s * q,
        1.0 - r - s * p + s * d - t * q,
        -s * p - t * d,
        t * p,
    )


def kernel(dims, *refs):
    levels, rows, cells, width, n_lon, n_lat, step = dims
    chunks = chunk_list(levels, rows, step)
    nq = len(chunks)
    tr, ad, shifts_in, fractions_in, mer_in, of, oa = refs[:7]
    gath = (refs[7 : 7 + nq], refs[7 + nq : 7 + 2 * nq])
    zb, ab, vb, taps, shifts, fractions, mer, held, loc, ssem, rsem, hs, hr, vs, vr = refs[7 + 2 * nq :]
    total_cells = cells * n_lon
    total_rows = rows * n_lat
    n_x = n_lon // 2

    me = lax.axis_index("lon")
    lat = lax.axis_index("lat")
    first = lat * rows
    core = lax.rem(me, 2)
    partner = me + 1 - 2 * core
    via = n_lon == 5 and n_lat == 4 and nq >= 4
    half = nq // 2
    detour = [half - 2, half - 1] if via else []
    if via:
        order = list(range(half - 2)) + list(range(half, nq - 2)) + detour + [nq - 2, nq - 1]
    else:
        order = list(range(nq))
    mate = lat + 1 - 2 * lax.rem(lat, 2)
    across = {"lon": lax.rem(me + 2, n_lon), "lat": mate}
    helper = jnp.logical_and(lat > 0, lat < n_lat - 1)
    helped = jnp.logical_not(helper)

    own = []
    dup = []
    for q, (lv, r0) in enumerate(chunks):
        a = pltpu.make_async_copy(
            tr.at[lv, pl.ds(r0, step)], gath[0][q].at[:, pl.ds(0, cells)], loc.at[q]
        )
        a.start()
        own.append(a)
    adc = pltpu.make_async_copy(ad, ab.at[:, pl.ds(RIM, rows)], loc.at[2 * nq])
    adc.start()
    for q, (lv, r0) in enumerate(chunks):
        b = pltpu.make_async_copy(
            tr.at[lv, pl.ds(r0, step)],
            gath[0][q].at[:, pl.ds(total_cells, cells)],
            loc.at[nq + q],
        )
        b.start()
        dup.append(b)

    small = []
    for k, (source, target) in enumerate(
        ((shifts_in, shifts), (fractions_in, fractions), (mer_in, mer))
    ):
        d = pltpu.make_async_copy(source, target, loc.at[2 * nq + 1 + k])
        d.start()
        small.append(d)

    barrier = pltpu.get_barrier_semaphore()
    pl.semaphore_signal(barrier, inc=1, device_id={"lon": partner}, device_id_type=MESH)
    for dx in range(1, n_x):
        pl.semaphore_signal(
            barrier, inc=1, device_id={"lon": lax.rem(me + 2 * dx, n_lon)}, device_id_type=MESH
        )

    if via:
        pl.semaphore_signal(barrier, inc=1, device_id=across, device_id_type=MESH)

    @pl.when(lat > 0)
    def _():
        pl.semaphore_signal(barrier, inc=1, device_id={"lat": lat - 1}, device_id_type=MESH)

    @pl.when(lat < n_lat - 1)
    def _():
        pl.semaphore_signal(barrier, inc=1, device_id={"lat": lat + 1}, device_id_type=MESH)

    inner = jnp.logical_and(lat > 0, lat < n_lat - 1)

    @pl.when(inner)
    def _():
        pl.semaphore_wait(barrier, n_x + 2 + int(via))

    @pl.when(jnp.logical_not(inner))
    def _():
        pl.semaphore_wait(barrier, n_x + min(n_lat - 1, 1) + int(via))

    def lat_copies(buf, k):
        down = pltpu.make_async_remote_copy(
            buf.at[:, pl.ds(RIM, RIM)],
            buf.at[:, pl.ds(RIM + rows, RIM)],
            hs.at[k, 0],
            hr.at[k, 0],
            device_id={"lat": lat - 1},
            device_id_type=MESH,
        )
        up = pltpu.make_async_remote_copy(
            buf.at[:, pl.ds(rows, RIM)],
            buf.at[:, pl.ds(0, RIM)],
            hs.at[k, 1],
            hr.at[k, 1],
            device_id={"lat": lat + 1},
            device_id_type=MESH,
        )
        return down, up

    def lat_start(buf, k):
        down, up = lat_copies(buf, k)

        @pl.when(lat > 0)
        def _():
            down.start()

        @pl.when(lat < n_lat - 1)
        def _():
            up.start()

    def lat_wait(buf, k):
        down, up = lat_copies(buf, k)

        @pl.when(lat > 0)
        def _():
            down.wait_send()
            up.wait_recv()

        @pl.when(lat < n_lat - 1)
        def _():
            up.wait_send()
            down.wait_recv()

    def x_copy(a, q, dx, span):
        lo, hi = span
        return pltpu.make_async_remote_copy(
            gath[a][q].at[:, pl.ds(lo, hi - lo)],
            gath[a][q].at[:, pl.ds((n_lon - 2 * dx) * cells + lo, hi - lo)],
            ssem.at[a, q, dx],
            rsem.at[a, q, dx],
            device_id={"lon": lax.rem(me + 2 * dx, n_lon)},
            device_id_type=MESH,
        )

    def core_copy(a, q, dx, span):
        lo, hi = span
        source = ((n_lon - 2 * dx) % n_lon) * cells + lo
        slot = lax.rem(2 * n_lon - 2 * dx + 2 * core - 1, n_lon)
        return pltpu.make_async_remote_copy(
            gath[a][q].at[:, pl.ds(source, hi - lo)],
            gath[a][q].at[:, pl.ds(pl.multiple_of(slot * cells + lo, SUB), hi - lo)],
            ssem.at[a, q, n_x + dx],
            rsem.at[a, q, n_x + dx],
            device_id={"lon": partner},
            device_id_type=MESH,
        )

    def out_copy(a, q):
        i = detour.index(q)
        return pltpu.make_async_remote_copy(
            gath[a][q].at[:, pl.ds(0, cells)],
            held.at[a, i],
            vs.at[a, i, 0],
            vr.at[a, i, 0],
            device_id=across if ROUTE else {"lat": mate},
            device_id_type=MESH,
        )

    def on_copy(a, q):
        i = detour.index(q)
        return pltpu.make_async_remote_copy(
            held.at[a, i],
            gath[a][q].at[:, pl.ds((n_lon - 2) * cells, cells)],
            vs.at[a, i, 1],
            vr.at[a, i, 1],
            device_id={"lat": mate} if ROUTE else across,
            device_id_type=MESH,
        )

    whole = (0, cells)

    def by_span(a, q, who, act):
        groups = {}
        for z in range(n_lat):
            for k in range(2):
                groups.setdefault(span_of(dims, a, chunks[q][1], z, k), []).append((z, k))
        if len(groups) == 1:
            act(next(iter(groups)))
            return
        for span, places in groups.items():
            hit = None
            for z in range(n_lat):
                ks = [k for y, k in places if y == z]
                if not ks:
                    continue
                here = lat == z
                if len(ks) == 1:
                    here = jnp.logical_and(here, who == ks[0])
                hit = here if hit is None else jnp.logical_or(hit, here)

            @pl.when(hit)
            def _():
                act(span)

    def direct(a, q, act):
        if q in detour:

            @pl.when(helper)
            def _():
                by_span(a, q, core, act)

        else:
            by_span(a, q, core, act)

    def detoured(q, act):
        if q in detour:

            @pl.when(helped)
            def _():
                act()

    def gather_start(a, q):
        detoured(q, lambda: out_copy(a, q).start())
        for dx in range(1, n_x):
            direct(a, q, lambda span: x_copy(a, q, dx, span).start())
        core_copy(a, q, 0, whole).start()

    def pass_on(a):
        for q in detour:

            @pl.when(helper)
            def _():
                out_copy(a, q).wait_recv()
                on_copy(a, q).start()

    def relay(a, q):
        def ready():
            on_copy(a, q).wait_recv()
            core_copy(a, q, 1, whole).start()

        detoured(q, ready)
        for dx in range(1, n_x):

            def act(span):
                x_copy(a, q, dx, span).wait_recv()
                core_copy(a, q, dx, span).start()

            direct(a, q, act)

    def gather_finish(a, q):
        core_copy(a, q, 0, whole).wait_recv()
        for dx in range(1, n_x):
            by_span(a, q, 1 - core, lambda span: core_copy(a, q, dx, span).wait_recv())

    def gather_drain(a, q):
        detoured(q, lambda: out_copy(a, q).wait_send())
        if q in detour:

            @pl.when(helper)
            def _():
                on_copy(a, q).wait_send()

        core_copy(a, q, 0, whole).wait_send()
        for dx in range(1, n_x):
            direct(a, q, lambda span: x_copy(a, q, dx, span).wait_send())
            by_span(a, q, core, lambda span: core_copy(a, q, dx, span).wait_send())

    adc.wait()
    lat_start(ab, 0)
    for q in range(nq):
        own[q].wait()
        gather_start(0, q)

    @pl.when(lat == 0)
    def _():
        for buf in (ab, zb):
            buf[:, pl.ds(0, RIM)] = jnp.zeros((levels, RIM, cells, width), jnp.float32)

    @pl.when(lat == n_lat - 1)
    def _():
        for buf in (ab, zb):
            buf[:, pl.ds(RIM + rows, RIM)] = jnp.zeros((levels, RIM, cells, width), jnp.float32)

    for d in small:
        d.wait()
    faces = rows + 5
    lanes = lax.broadcasted_iota(jnp.int32, (cells, total_rows), 1)
    for lv in range(levels):

        @pl.loop(0, faces)
        def _(f):
            row = first + f - 2
            chosen = jnp.logical_and(lanes == row, lanes > 0)
            column = jnp.sum(jnp.where(chosen, mer[lv], 0.0), axis=1, keepdims=True)
            vb[lv, f] = jnp.broadcast_to(column, (cells, width))

        @pl.loop(0, rows)
        def _(r):
            for k, t in enumerate(zonal_taps(fractions[lv, first + r])):
                taps[(lv * rows + r) * 6 + k] = t

    pass_on(0)

    lat_wait(ab, 0)
    for lv in range(levels):

        @pl.loop(0, cells // SUB)
        def _(c):
            at = pl.ds(pl.multiple_of(c * SUB, SUB), SUB)
            ev, q6b, dqb, eb = {}, {}, {}, {}
            carry = None
            y = {r: ab[lv, r + RIM, at, :] for r in range(-3, -1)}
            for f in range(-2, rows + 3):
                y[f] = ab[lv, f + RIM, at, :]
                v = vb[lv, f + 2, at, :]
                north = v > 0.0
                beta, gamma = face_terms(v)
                change = y[f] - y[f - 1]
                ev[f] = v * change
                b = beta * change
                g = -gamma * change
                bn, gn = jnp.where(north, b, 0.0), jnp.where(north, g, 0.0)
                if carry is not None:
                    q6b[f - 1] = bn + carry[0]
                    dqb[f - 1] = gn + carry[1]
                carry = (b - bn, g - gn)
                h = f - 1
                if h >= -1:
                    eb[h] = ev[h] - 3.0 * (q6b[h - 1] + q6b[h]) + (dqb[h - 1] - dqb[h])
                r = h - 2
                if r >= 0:
                    value = (
                        y[r]
                        + 6.0 * q6b[r]
                        + (7.0 / 12.0) * (eb[r] + eb[r + 1])
                        - (1.0 / 12.0) * (eb[r - 1] + eb[r + 2])
                    )
                    q = lv * (rows // step) + r // step
                    gath[1][q][r % step, at, :] = value
                    gath[1][q][
                        r % step, pl.ds(pl.multiple_of(total_cells + c * SUB, SUB), SUB), :
                    ] = value

        if lv == levels - 1:
            pass_on(1)
        for q, (l2, _r) in enumerate(chunks):
            if l2 == lv:
                gather_start(1, q)

    def sweep(a, q, sink, sink_row, sign):
        lv, r0 = chunks[q]
        buf = gath[a][q]

        @pl.loop(0, step)
        def _(r):
            buf[r, pl.ds(total_cells + cells, SUB), :] = buf[r, pl.ds(cells, SUB), :]
            shift = shifts[lv, first + r0 + r]
            if sign < 0:
                start = lax.rem(2 * total_cells - shift - 3, total_cells)
            else:
                start = lax.rem(2 * total_cells + shift - 2, total_cells)
            base = (lv * rows + r0 + r) * 6
            w = [taps[base + k] for k in range(6)]
            if sign > 0:
                w = w[::-1]
            for c in range(cells // SUB):
                total = None
                for k in range(6):
                    term = w[k] * buf[r, pl.ds(start + c * SUB + k, SUB), :]
                    total = term if total is None else total + term
                sink[lv, sink_row + r0 + r, pl.ds(c * SUB, SUB), :] = total

    for b in dup:
        b.wait()
    for i, q in enumerate(order):
        relay(0, q)
        if i > 0:
            gather_finish(0, order[i - 1])
            sweep(0, order[i - 1], zb, RIM, -1)
    gather_finish(0, order[-1])
    sweep(0, order[-1], zb, RIM, -1)
    lat_start(zb, 1)

    relay(1, order[0])
    lat_wait(zb, 1)

    for lv in range(levels):

        @pl.loop(0, cells // SUB)
        def _(c):
            at = pl.ds(pl.multiple_of(c * SUB, SUB), SUB)
            z = {r: zb[lv, r + RIM, at, :] for r in range(-3, 0)}
            e, q6, dq, flux = {}, {}, {}, {}
            for f in range(-1, rows + 2):
                z[f + 1] = zb[lv, f + 1 + RIM, at, :]
                e[f] = (7.0 / 12.0) * (z[f - 1] + z[f]) - (1.0 / 12.0) * (z[f - 2] + z[f + 1])
                u = f - 1
                if u >= -1:
                    q6[u] = 6.0 * z[u] - 3.0 * (e[u] + e[f])
                    dq[u] = e[f] - e[u]
                if u >= 0:
                    v = vb[lv, u + 2, at, :]
                    north = v > 0.0
                    beta, gamma = face_terms(v)
                    flux[u] = (
                        v * e[u]
                        + beta * jnp.where(north, q6[u - 1], q6[u])
                        - gamma * jnp.where(north, dq[u - 1], dq[u])
                    )
                if u >= 1:
                    of[lv, u - 1, at, :] = z[u - 1] - flux[u] + flux[u - 1]

    def finish_adjoint(q):
        lv, r0 = chunks[q]
        gather_finish(1, q)
        sweep(1, q, oa, 0, 1)

    for i in range(1, nq):
        relay(1, order[i])
        finish_adjoint(order[i - 1])
    finish_adjoint(order[-1])

    for a in range(2):
        for q in range(nq):
            gather_drain(a, q)


def local(tracers, adjoint_in, shifts, fractions, meridional):
    levels, rows, cells, width = tracers.shape
    n_lon, n_lat = lax.axis_size("lon"), lax.axis_size("lat")
    step = max(1, rows // 2)
    nq = levels * (rows // step)
    n_x = n_lon // 2
    dims = (levels, rows, cells, width, n_lon, n_lat, step)
    block = pltpu.VMEM((step, (n_lon + 1) * cells + SUB, width), jnp.float32)
    banded = pltpu.VMEM((levels, rows + 2 * RIM, cells, width), jnp.float32)
    vmem = pl.BlockSpec(memory_space=pltpu.VMEM)
    far = pl.BlockSpec(memory_space=pltpu.HBM)
    shape = jax.ShapeDtypeStruct(tracers.shape, jnp.float32)
    return pl.pallas_call(
        functools.partial(kernel, dims),
        out_shape=(shape, shape),
        in_specs=[far] * 5,
        out_specs=(vmem, vmem),
        scratch_shapes=[block] * (2 * nq)
        + [
            banded,
            banded,
            pltpu.VMEM((levels, rows + 5, cells, width), jnp.float32),
            pltpu.SMEM((levels * rows * 6,), jnp.float32),
            pltpu.SMEM(shifts.shape, jnp.int32),
            pltpu.SMEM(fractions.shape, jnp.float32),
            pltpu.VMEM((levels, cells, meridional.shape[1]), jnp.float32),
            pltpu.VMEM((2, 2, step, cells, width), jnp.float32),
            pltpu.SemaphoreType.DMA((2 * nq + 4,)),
            pltpu.SemaphoreType.DMA((2, nq, 2 * n_x)),
            pltpu.SemaphoreType.DMA((2, nq, 2 * n_x)),
            pltpu.SemaphoreType.DMA((2, 2)),
            pltpu.SemaphoreType.DMA((2, 2)),
            pltpu.SemaphoreType.DMA((2, 2, 2)),
            pltpu.SemaphoreType.DMA((2, 2, 2)),
        ],
        compiler_params=pltpu.CompilerParams(
            collective_id=0, has_side_effects=True, vmem_limit_bytes=60 << 20
        ),
    )(tracers, adjoint_in, shifts, fractions, jnp.swapaxes(meridional, 1, 2))


def solution(mesh):
    block = P("grp", "lat", "lon", None)
    in_specs = (block, block, P(), P(), P(None, None, "lon"))
    return jax.shard_map(
        local, mesh=mesh, in_specs=in_specs, out_specs=(block, block), check_vma=False
    )
```
